32 devices in a mesh: rows: 8 (over y, x, core), grp: 4 (over z).
Axes of the slice: x: 2, y: 2, z: 4, core: 2. Of those that a mesh axis runs over, the one named last changes fastest.
Arguments:
- factor: float32 [8192, 1024], P(('rows', 'grp')), as said below
- start_block: float32 [1024, 256], replicated, may hold values from -6 to 6
Outputs:
- compressed: float32 [8192, 256], P(('rows', 'grp'))
- tail_share: float32 [], replicated
The draws below stay inside these ranges and needn't reach their ends.
Inputs may be any that keep to these rules, and one draw needn't show every extreme that they name: Every entry is finite; the factor has full column rank.
All inputs are finite; a program needn't handle non-finite values.
Results may differ from the reference program's by a relative error of at most 0.0007.
Values sent between devices are 32-bit elements; how exact they have to be, the bound alone decides.
No kernel may reach another device: no remote copies, remote signals or barrier semaphores. Data moves between devices by JAX's collectives and lax.ppermute only.
A program may use at most 64 MiB of HBM per device.

```python
import math
import jax
import jax.numpy as jnp
from jax import lax

K = 1024
RANK = 256
ITERS = 1
ROWS_ALL = 8192


def draw_factor(key, part):
    keys = jax.random.split(key, 3)
    position = jnp.arange(ROWS_ALL, dtype=jnp.float32) / ROWS_ALL
    row_scale = jnp.exp(jax.random.uniform(keys[0], (ROWS_ALL,), jnp.float32) * math.log(10.0)) * (1.0 + 2.0 * position)
    col_scale = jnp.exp(jax.random.uniform(keys[1], (K,), jnp.float32) * math.log(10.0))
    noise = jax.random.normal(keys[2], (ROWS_ALL, K), jnp.float32)
    return (0.1 * row_scale[:, None] * col_scale[None, :] * noise).astype(jnp.float32)


def normal_values(own_key, shape, width, reach, kind=jnp.bfloat16):
    array = jax.random.normal(own_key, shape, jnp.float32) * width
    return jnp.minimum(jnp.maximum(array, -reach), reach).astype(kind)


def setup_inputs(seed: int = 0) -> dict:
    streams_of = jax.random.split(jax.random.key(seed), 3)
    return {
        "factor": draw_factor(jax.random.fold_in(streams_of[2], 71), 0),
        "start_block": normal_values(streams_of[1], (K, RANK), 1.0, 6.0, jnp.float32),
    }


def orthonormal(columns):
    product = jnp.dot(columns.T, columns, precision=lax.Precision.HIGHEST)
    lower_factor = jnp.linalg.cholesky(product)
    return jax.scipy.linalg.solve_triangular(lower_factor, columns.T, lower=True).T

def reference(factor, start_block):
    gram_total = jnp.dot(factor.T, factor, precision=lax.Precision.HIGHEST)
    basis_now = orthonormal(start_block)
    for iteration in range(ITERS):
        basis_now = orthonormal(jnp.dot(gram_total, basis_now, precision=lax.Precision.HIGHEST))
    compressed = jnp.dot(factor, basis_now, precision=lax.Precision.HIGHEST)
    kept_energy = jnp.sum(basis_now * jnp.dot(gram_total, basis_now, precision=lax.Precision.HIGHEST))
    total_energy = jnp.trace(gram_total)
    tail_share = (1.0 - kept_energy / total_energy).astype(jnp.float32)
    return (compressed, tail_share)
```

```python
import functools
import jax
import jax.numpy as jnp
from jax import lax
from jax.experimental import pallas as pl
from jax.experimental.pallas import tpu as pltpu
from jax.sharding import PartitionSpec as P

LANES = 128
PANEL = 32
EXACT = lax.Precision.HIGHEST
VMEM = pl.BlockSpec(memory_space=pltpu.VMEM)


def dot(a, b, contract=((1,), (0,))):
    return lax.dot_general(
        a, b, (contract, ((), ())), precision=EXACT, preferred_element_type=jnp.float32
    )


def split3(x):
    high = x.astype(jnp.bfloat16)
    rest = x - high.astype(jnp.float32)
    mid = rest.astype(jnp.bfloat16)
    low = (rest - mid.astype(jnp.float32)).astype(jnp.bfloat16)
    return high, mid, low


def eliminate(m, out, n):
    width = m.shape[1]
    b = PANEL
    for r0 in range(0, n, b):
        lo = r0 // LANES * LANES
        chunks = list(range(lo, width, LANES))
        diag = m[r0 : r0 + b, lo : lo + LANES]
        cols = [jnp.broadcast_to(diag[:, r0 - lo + j : r0 - lo + j + 1], (b, LANES)) for j in range(b)]
        rows = [m[r0 : r0 + b, q : q + LANES] for q in chunks]
        index = lax.broadcasted_iota(jnp.int32, (b, LANES), 0)
        solved = [[] for _ in chunks]
        for j in range(b):
            scale = lax.rsqrt(cols[j][j : j + 1, :])
            column = cols[j] * scale
            for k in range(j + 1, b):
                cols[k] = cols[k] - column * column[k : k + 1, :]
            below = jnp.where(index > j, column, 0.0)
            for q in range(len(chunks)):
                unit = rows[q][j : j + 1, :] * scale
                solved[q].append(unit)
                if j + 1 < b:
                    rows[q] = rows[q] - below * unit
        panel = [jnp.concatenate(s, axis=0) for s in solved]
        for q, start in enumerate(chunks):
            if start >= n:
                out[r0 : r0 + b, start - n : start - n + LANES] = panel[q]
        done = r0 + b
        if done < n:
            lo2 = done // LANES * LANES
            keep = [panel[q] for q, start in enumerate(chunks) if start >= lo2]
            block = jnp.concatenate(keep, axis=1)
            high, mid, low = split3(block)
            span = n - lo2
            left = jnp.concatenate([v[:, :span] for v in (high, high, mid, high, mid, low)], axis=0)
            right = jnp.concatenate([high, mid, high, low, mid, high], axis=0)
            update = lax.dot_general(
                left, right, (((0,), (0,)), ((), ())), preferred_element_type=jnp.float32
            )
            m[done:n, lo2:width] = m[done:n, lo2:width] - update[done - lo2 :, :]


def start_kernel(axis, parts, z_ref, s_ref, *refs):
    outs, whole = refs[:-1], refs[-1]
    me = lax.axis_index(axis)
    image = dot(z_ref[...], s_ref[...])
    whole[...] = dot(image.T, z_ref[...])
    block = whole.shape[1] // parts
    for r in range(parts):
        place = pl.multiple_of(jnp.bitwise_xor(me & (parts - 1), r) * block, LANES)
        outs[r % 2][r // 2] = whole[:, pl.ds(place, block)]


def first_kernel(s_ref, out_ref, m):
    n = s_ref.shape[1]
    s = s_ref[...]
    m[:, :n] = dot(s.T, s)
    index = lax.broadcasted_iota(jnp.int32, (n, n), 0)
    other = lax.broadcasted_iota(jnp.int32, (n, n), 1)
    m[:, n:] = jnp.where(index == other, 1.0, 0.0)
    eliminate(m, out_ref, n)


def shard_kernel(inverse_ref, *refs):
    total = refs[0][...]
    for ref in refs[1:-1]:
        total = total + ref[...]
    refs[-1][...] = dot(inverse_ref[...], total)


def last_kernel(axis, parts, z_ref, near_ref, far_ref, out_ref, energy_ref, whole, m, solved):
    me = lax.axis_index(axis)
    n = near_ref.shape[1]
    block = near_ref.shape[2]
    for r in range(parts):
        place = pl.multiple_of(jnp.bitwise_xor(me & (parts - 1), r) * block, LANES)
        whole[:, pl.ds(place, block)] = (near_ref, far_ref)[r % 2][r // 2]
    y = whole[...]
    z = z_ref[...]
    m[:, :n] = dot(y, y, ((1,), (1,)))
    m[:, n:] = dot(y, z, ((1,), (1,)))
    eliminate(m, solved, n)
    result = solved[...]
    out_ref[...] = result.T
    kept = jnp.sum(result * result)
    total = jnp.sum(z * z)
    lane = lax.broadcasted_iota(jnp.int32, energy_ref.shape, 2)
    energy_ref[...] = jnp.where(lane == 0, kept, jnp.where(lane == 1, total, 0.0))


def call(kernel, outs, scratch, flops, name):
    shapes = [jax.ShapeDtypeStruct(s, jnp.float32) for s in outs]
    moved = 4 * sum(functools.reduce(lambda a, b: a * b, s, 1) for s in outs)
    return pl.pallas_call(
        kernel,
        out_shape=shapes,
        out_specs=[VMEM] * len(outs),
        scratch_shapes=[pltpu.VMEM(s, jnp.float32) for s in scratch],
        cost_estimate=pl.CostEstimate(flops=flops, bytes_accessed=moved, transcendentals=0),
        name=name,
    )


def exchange(x, axis, size, mask):
    return lax.ppermute(x, axis, [(i, i ^ mask) for i in range(size)])


def local(rows_size, grp_size, factor, start_block):
    own, k = factor.shape
    n = start_block.shape[1]
    parts = min(rows_size, k // LANES)
    block = k // parts
    half = parts // 2
    vm = lambda count: [VMEM] * count

    keep, send = call(
        functools.partial(start_kernel, "rows", parts),
        [(half, n, block)] * 2, [(n, k)], 10**8, "image",
    )(factor, start_block)
    (inverse,) = call(first_kernel, [(n, n)], [(n, 2 * n)], 4 * 10**9, "first")(start_block)

    got = exchange(send, "rows", rows_size, 1)
    pieces = [keep[i] + got[i] for i in range(half)]
    total = pieces[0]
    moved = [exchange(pieces[i], "rows", rows_size, 2 * i) for i in range(1, half)]
    for piece in moved:
        total = total + piece
    masks = [("rows", rows_size, 1 << i) for i in range(parts.bit_length() - 1, rows_size.bit_length() - 1)]
    masks += [("grp", grp_size, 1 << i) for i in range(grp_size.bit_length() - 1)]
    terms = [total]
    for axis, size, mask in masks:
        total = sum(terms[1:], terms[0])
        terms = [total, exchange(total, axis, size, mask)]
    (shard,) = call(shard_kernel, [(n, block)], [], 10**8, "shard")(inverse, *terms)

    near = jnp.stack([shard] + [exchange(shard, "rows", rows_size, 2 * i) for i in range(1, half)])
    far = exchange(near, "rows", rows_size, 1)
    count = rows_size * grp_size
    compressed, energy = call(
        functools.partial(last_kernel, "rows", parts),
        [(own, n), (count, 1, LANES)], [(n, k), (n, 2 * n), (n, n)], 4 * 10**9, "last",
    )(factor, near, far)
    energy = lax.all_to_all(energy, ("rows", "grp"), 0, 0, tiled=True)
    energy = jnp.sum(energy, axis=(0, 1))
    tail_share = (1.0 - energy[0] / energy[1]).astype(jnp.float32)
    return compressed, tail_share


def solution(mesh):
    body = functools.partial(local, mesh.shape["rows"], mesh.shape["grp"])
    return jax.shard_map(
        body,
        mesh=mesh,
        in_specs=(P(("rows", "grp"), None), P()),
        out_specs=(P(("rows", "grp"), None), P()),
        check_vma=False,
    )
```

```python
import functools
import math
import jax
import jax.numpy as jnp
from jax import lax
from jax.experimental import pallas as pl
from jax.experimental.pallas import tpu as pltpu
from jax.sharding import PartitionSpec as P

LANES = 128
PANEL = 32
EXACT = lax.Precision.HIGHEST
VMEM = pl.BlockSpec(memory_space=pltpu.VMEM)
HBM = pl.BlockSpec(memory_space=pltpu.HBM)


def dot(a, b, contract=((1,), (0,))):
    return lax.dot_general(
        a, b, (contract, ((), ())), precision=EXACT, preferred_element_type=jnp.float32
    )


def split3(x):
    high = x.astype(jnp.bfloat16)
    rest = x - high.astype(jnp.float32)
    mid = rest.astype(jnp.bfloat16)
    low = (rest - mid.astype(jnp.float32)).astype(jnp.bfloat16)
    return high, mid, low


def eliminate(m, out, n, first, last, lower):
    width = m.shape[1]
    b = PANEL
    group = lax.broadcasted_iota(jnp.int32, (8, LANES), 0)
    for r0 in range(first, last, b):
        lo = r0 // LANES * LANES
        end = n + lo + LANES if lower else width
        chunks = list(range(lo, end, LANES))
        diag = m[r0 : r0 + b, lo : lo + LANES]
        cols = [
            jnp.broadcast_to(diag[j // 8 * 8 :, r0 - lo + j : r0 - lo + j + 1], (b - j // 8 * 8, LANES))
            for j in range(b)
        ]
        rows = [m[r0 : r0 + b, q : q + LANES] for q in chunks]
        solved = [[] for _ in chunks]
        for j in range(b):
            base = j // 8 * 8
            at = j - base
            scale = lax.rsqrt(cols[j][at : at + 1, :])
            column = cols[j] * scale
            for k in range(j + 1, b):
                skip = k // 8 * 8 - base
                cols[k] = cols[k] - column[skip:, :] * column[k - base : k - base + 1, :]
            head = jnp.where(group > at, column[:8, :], 0.0)
            below = jnp.concatenate([head, column[8:, :]], axis=0) if base + 8 < b else head
            for q in range(len(chunks)):
                unit = rows[q][at : at + 1, :] * scale
                solved[q].append(unit)
                if j + 1 < b:
                    rows[q] = rows[q] - below * unit
                    if at == 7:
                        rows[q] = rows[q][8:, :]
        panel = [jnp.concatenate(s, axis=0) for s in solved]
        for q, start in enumerate(chunks):
            if start >= n:
                out[r0 : r0 + b, start - n : start - n + LANES] = panel[q]
        if lower and end < width:
            out[r0 : r0 + b, end - n :] = jnp.zeros((b, width - end), jnp.float32)
        done = r0 + b
        if done < n:
            lo2 = done // LANES * LANES
            block = jnp.concatenate(panel[(lo2 - lo) // LANES :], axis=1)
            high, mid, low = split3(block)
            span = n - lo2
            left = jnp.concatenate([v[:, :span] for v in (high, high, mid, high, mid, low)], axis=0)
            right = jnp.concatenate([high, mid, high, low, mid, high], axis=0)
            update = lax.dot_general(
                left, right, (((0,), (0,)), ((), ())), preferred_element_type=jnp.float32
            )
            m[done:n, lo2:end] = m[done:n, lo2:end] - update[done - lo2 :, :]


def place_of(axes, parts, block, r):
    rows, grp = lax.axis_index(axes[0]), lax.axis_index(axes[1])
    flip = grp & 1
    for bit in range(1, 8):
        flip = flip ^ ((grp >> bit) & 1)
    me = (rows & (parts - 1)) ^ flip
    return pl.multiple_of((me ^ r) * block, LANES)


def pair(x):
    high = x.astype(jnp.bfloat16)
    return high, (x - high.astype(jnp.float32)).astype(jnp.bfloat16)


def dot3(a, b, contract=((1,), (0,))):
    (ah, al), (bh, bl) = a, b
    left = jnp.concatenate([ah, ah, al], axis=contract[0][0])
    right = jnp.concatenate([bh, bl, bh], axis=contract[1][0])
    return lax.dot_general(left, right, (contract, ((), ())), preferred_element_type=jnp.float32)


def start_kernel(axes, parts, kept, z_hbm, s_hbm, keep_ref, send_ref, whole, z_ref, s_ref, sems):
    k = z_ref.shape[1]
    step = min(k, 2 * LANES)
    copies = []
    for i in range(k // step):
        span = pl.ds(i * step, step)
        copies.append((
            pltpu.make_async_copy(z_hbm.at[:, span], z_ref.at[:, span], sems.at[2 * i]),
            pltpu.make_async_copy(s_hbm.at[span, :], s_ref.at[span, :], sems.at[2 * i + 1]),
        ))
        for copy in copies[-1]:
            copy.start()
    image, halves = 0.0, []
    for i, both in enumerate(copies):
        for copy in both:
            copy.wait()
        halves.append(pair(z_ref[:, i * step : (i + 1) * step]))
        image = image + dot3(halves[i], pair(s_ref[i * step : (i + 1) * step, :]))
    turned = pair(image.T)
    for i, z in enumerate(halves):
        whole[:, i * step : (i + 1) * step] = dot3(turned, z)
    block = k // parts
    for i, r in enumerate(kept):
        keep_ref[i] = whole[:, pl.ds(place_of(axes, parts, block, r), block)]
        send_ref[i] = whole[:, pl.ds(place_of(axes, parts, block, r ^ 1), block)]


def first_kernel(s_ref, m_ref, out_ref):
    n = s_ref.shape[1]
    s = s_ref[...]
    m_ref[:, :n] = dot(s.T, s)
    index = lax.broadcasted_iota(jnp.int32, (n, n), 0)
    other = lax.broadcasted_iota(jnp.int32, (n, n), 1)
    m_ref[:, n:] = jnp.where(index == other, 1.0, 0.0)
    eliminate(m_ref, out_ref, n, 0, n // 2, True)


def second_kernel(m_ref, half_ref, z_ref, out_ref, total_ref, m):
    n = m.shape[0]
    m[n // 2 :, :] = m_ref[n // 2 :, :]
    out_ref[: n // 2, :] = half_ref[: n // 2, :]
    eliminate(m, out_ref, n, n // 2, n, True)
    z = z_ref[...]
    total_ref[...] = jnp.sum(z * z, axis=0, keepdims=True)


def shard_kernel(inverse_ref, *refs):
    total = refs[0][...]
    for ref in refs[1:-1]:
        total = total + ref[...]
    refs[-1][...] = dot(inverse_ref[...], total)


def products(axes, parts, numbers, z_ref, y_ref):
    block = y_ref.shape[2]
    y = jnp.concatenate([y_ref[i] for i in range(len(numbers))], axis=1)
    z = jnp.concatenate(
        [z_ref[:, pl.ds(place_of(axes, parts, block, r), block)] for r in numbers], axis=1
    )
    across = ((1,), (1,))
    return dot(y, y, across), dot3(pair(y), pair(z), across)


def near_kernel(axes, parts, kept, z_ref, near_ref, m_ref):
    n = m_ref.shape[0]
    m_ref[:, :n], m_ref[:, n:] = products(axes, parts, kept, z_ref, near_ref)


def last_kernel(axes, parts, kept, z_ref, near_ref, far_ref, total_ref, out_hbm, energy_ref, m, solved, out, sems):
    n = near_ref.shape[0]
    gram, image = products(axes, parts, [r ^ 1 for r in kept], z_ref, far_ref)
    m[:, :n] = near_ref[:, :n] + gram
    m[:, n:] = near_ref[:, n:] + image
    half = n // 2
    copies, energy = [], 0.0
    for i in range(2):
        span = pl.ds(i * half, half)
        eliminate(m, solved, n, i * half, (i + 1) * half, False)
        result = solved[i * half : (i + 1) * half, :]
        out[:, i * half : (i + 1) * half] = result.T
        copies.append(pltpu.make_async_copy(out.at[:, span], out_hbm.at[:, span], sems.at[i]))
        copies[i].start()
        energy = energy + jnp.sum(result * result)
    lane = lax.broadcasted_iota(jnp.int32, energy_ref.shape, 2)
    total = jnp.sum(total_ref[...])
    energy_ref[...] = jnp.where(lane == 0, energy, jnp.where(lane == 1, total, 0.0))
    for copy in copies:
        copy.wait()


def share_kernel(energy_ref, out_ref):
    sums = jnp.sum(energy_ref[:, 0, :], axis=0, keepdims=True)
    out_ref[...] = 1.0 - sums[:, 0:1] / sums[:, 1:2]


def call(kernel, outs, scratch, flops, name, limit, in_hbm=(), out_hbm=()):
    moved = 4 * sum(math.prod(s) for s in outs)

    def run(*args):
        return pl.pallas_call(
            kernel,
            out_shape=[jax.ShapeDtypeStruct(s, jnp.float32) for s in outs],
            in_specs=[HBM if i in in_hbm else VMEM for i in range(len(args))],
            out_specs=[HBM if i in out_hbm else VMEM for i in range(len(outs))],
            scratch_shapes=[
                pltpu.SemaphoreType.DMA((s,)) if isinstance(s, int) else pltpu.VMEM(s, jnp.float32)
                for s in scratch
            ],
            cost_estimate=pl.CostEstimate(flops=flops, bytes_accessed=moved, transcendentals=0),
            compiler_params=pltpu.CompilerParams(vmem_limit_bytes=limit * 2**20),
            name=name,
        )(*args)

    return run


def exchange(x, axis, size, mask):
    return lax.ppermute(x, axis, [(i, i ^ mask) for i in range(size)])


def steps_over(rows_size, grp_size, parts):
    masks = [(1 << i, 0) for i in range(parts.bit_length() - 1, rows_size.bit_length() - 1)]
    masks += [(1, 1 << i) for i in range(grp_size.bit_length() - 1)]
    def pairs(position):
        out = []
        for r in range(rows_size):
            for g in range(grp_size):
                odd = (r ^ bin(g).count("1")) & 1
                row_mask, grp_mask = masks[-1 - position] if odd else masks[position]
                out.append((r * grp_size + g, (r ^ row_mask) * grp_size + (g ^ grp_mask)))
        return out
    return [pairs(i) for i in range(len(masks))]


def local(rows_size, grp_size, factor, start_block):
    own, k = factor.shape
    n = start_block.shape[1]
    parts = min(rows_size, k // LANES)
    block = k // parts
    half = parts // 2
    axes = ("rows", "grp")
    kept = [0] + [2 * i + 1 for i in range(1, half)]
    tie = lax.optimization_barrier
    apart = pltpu.with_memory_space_constraint

    keep, send = call(
        functools.partial(start_kernel, axes, parts, kept),
        [(half, n, block)] * 2, [(n, k), (own, k), (k, n), 2 * (k // min(k, 2 * LANES))], 10**8, "image", 14, (0, 1),
    )(apart(factor, pltpu.HBM), apart(start_block, pltpu.HBM))
    got = exchange(send, "rows", rows_size, 1)
    pieces = [keep[i] + got[i] for i in range(half)]
    pieces[0], start_block = tie((pieces[0], start_block))
    moved = [exchange(pieces[i], "rows", rows_size, kept[i]) for i in range(1, half)]
    first = call(first_kernel, [(n, 2 * n), (n, n)], [], 10**10, "first", 8)(start_block)
    first, moved = tie((first, moved))
    total = sum(moved, pieces[0])
    terms = [total]
    for i, pairs in enumerate(steps_over(rows_size, grp_size, parts)):
        total = sum(terms[1:], terms[0])
        other = lax.ppermute(total, axes, pairs)
        if i == 0:
            inverse, energy = call(
                second_kernel, [(n, n), (1, k)], [(n, 2 * n)], 5 * 10**9, "second", 8
            )(*first, factor)
            inverse, other = tie((inverse, other))
        terms = [total, other]
    (shard,) = call(shard_kernel, [(n, block)], [], 10**8, "shard", 4)(inverse, *terms)

    near = jnp.stack([shard] + [exchange(shard, "rows", rows_size, r) for r in kept[1:]])
    far = exchange(near, "rows", rows_size, 1)
    (begun,) = call(
        functools.partial(near_kernel, axes, parts, kept), [(n, n + own)], [], 10**9, "near", 8
    )(factor, near)
    begun, far = tie((begun, far))
    count = rows_size * grp_size
    compressed, energy = call(
        functools.partial(last_kernel, axes, parts, kept),
        [(own, n), (count, 1, LANES)], [(n, n + own), (n, own), (own, n), 2], 10**10, "last", 12, (), (0,),
    )(factor, begun, far, energy)
    energy = lax.all_to_all(energy, axes, 0, 0, tiled=True)
    (tail_share,) = call(share_kernel, [(1, 1)], [], 10**5, "share", 4)(energy)
    return compressed, tail_share.reshape(())


def solution(mesh):
    body = functools.partial(local, mesh.shape["rows"], mesh.shape["grp"])
    return jax.shard_map(
        body,
        mesh=mesh,
        in_specs=(P(("rows", "grp"), None), P()),
        out_specs=(P(("rows", "grp"), None), P()),
        check_vma=False,
    )
```

```python
import functools
import math
import jax
import jax.numpy as jnp
from jax import lax
from jax.experimental import pallas as pl
from jax.experimental.pallas import tpu as pltpu
from jax.sharding import PartitionSpec as P

LANES = 128
PANEL = 32
STRIP = 16
EXACT = lax.Precision.HIGHEST
VMEM = pl.BlockSpec(memory_space=pltpu.VMEM)
HBM = pl.BlockSpec(memory_space=pltpu.HBM)


def dot(a, b, contract=((1,), (0,))):
    return lax.dot_general(
        a, b, (contract, ((), ())), precision=EXACT, preferred_element_type=jnp.float32
    )


def split3(x):
    high = x.astype(jnp.bfloat16)
    rest = x - high.astype(jnp.float32)
    mid = rest.astype(jnp.bfloat16)
    low = (rest - mid.astype(jnp.float32)).astype(jnp.bfloat16)
    return high, mid, low


def eliminate(m, out, n, first, last, lower, cols):
    width = m.shape[1]
    b = PANEL
    group = lax.broadcasted_iota(jnp.int32, (8, LANES), 0)
    for r0 in range(first, last, b):
        lo = r0 // LANES * LANES
        end = n + lo + LANES if lower else width
        chunks = list(range(lo, end, LANES))
        solved = [[] for _ in chunks]
        for c0 in range(r0, r0 + b, STRIP):
            tall = r0 + b - c0
            for j in range(STRIP):
                top = j // 8 * 8
                entry = m[c0 + top : r0 + b, c0 + j : c0 + j + 1]
                cols[j, top:tall, :] = jnp.broadcast_to(entry, (tall - top, LANES))
            units = [[] for _ in chunks]
            for base in range(0, STRIP, 8):
                column = [cols[base + j, base:tall, :] for j in range(8)]
                rows = [m[c0 + base : c0 + base + 8, q : q + LANES] for q in chunks]
                for i in range(base):
                    factor = cols[i, base:tall, :]
                    for j in range(8):
                        column[j] = column[j] - factor * cols[i, base + j : base + j + 1, :]
                    for q in range(len(chunks)):
                        rows[q] = rows[q] - factor[:8, :] * units[q][i]
                for j in range(8):
                    scale = lax.rsqrt(column[j][j : j + 1, :])
                    column[j] = column[j] * scale
                    for k in range(j + 1, 8):
                        column[k] = column[k] - column[j] * column[j][k : k + 1, :]
                    if base + 8 < tall:
                        cols[base + j, base:tall, :] = column[j]
                    below = jnp.where(group > j, column[j][:8, :], 0.0)
                    for q in range(len(chunks)):
                        unit = rows[q][j : j + 1, :] * scale
                        units[q].append(unit)
                        if j < 7:
                            rows[q] = rows[q] - below * unit
            for q, start in enumerate(chunks):
                solved[q].append(jnp.concatenate(units[q], axis=0))
                for top in range(STRIP, tall, 8):
                    lower_rows = m[c0 + top : c0 + top + 8, start : start + LANES]
                    for i in range(STRIP):
                        lower_rows = lower_rows - cols[i, top : top + 8, :] * units[q][i]
                    m[c0 + top : c0 + top + 8, start : start + LANES] = lower_rows
        panel = [jnp.concatenate(s, axis=0) for s in solved]
        for q, start in enumerate(chunks):
            if start >= n:
                out[r0 : r0 + b, start - n : start - n + LANES] = panel[q]
        if lower and end < width:
            out[r0 : r0 + b, end - n :] = jnp.zeros((b, width - end), jnp.float32)
        done = r0 + b
        if done < n:
            lo2 = done // LANES * LANES
            block = jnp.concatenate(panel[(lo2 - lo) // LANES :], axis=1)
            high, mid, low = split3(block)
            span = n - lo2
            left = jnp.concatenate([v[:, :span] for v in (high, high, mid, high, mid, low)], axis=0)
            right = jnp.concatenate([high, mid, high, low, mid, high], axis=0)
            update = lax.dot_general(
                left, right, (((0,), (0,)), ((), ())), preferred_element_type=jnp.float32
            )
            m[done:n, lo2:end] = m[done:n, lo2:end] - update[done - lo2 :, :]


def place_of(axes, parts, block, r):
    rows, grp = lax.axis_index(axes[0]), lax.axis_index(axes[1])
    flip = grp & 1
    for bit in range(1, 8):
        flip = flip ^ ((grp >> bit) & 1)
    me = (rows & (parts - 1)) ^ flip
    return pl.multiple_of((me ^ r) * block, LANES)


def pair(x):
    high = x.astype(jnp.bfloat16)
    return high, (x - high.astype(jnp.float32)).astype(jnp.bfloat16)


def dot3(a, b, contract=((1,), (0,))):
    (ah, al), (bh, bl) = a, b
    left = jnp.concatenate([ah, ah, al], axis=contract[0][0])
    right = jnp.concatenate([bh, bl, bh], axis=contract[1][0])
    return lax.dot_general(left, right, (contract, ((), ())), preferred_element_type=jnp.float32)


def start_kernel(axes, parts, kept, z_hbm, s_hbm, keep_ref, send_ref, whole, z_ref, s_ref, sems):
    k = z_ref.shape[1]
    step = min(k, 2 * LANES)
    copies = []
    for i in range(k // step):
        span = pl.ds(i * step, step)
        copies.append((
            pltpu.make_async_copy(z_hbm.at[:, span], z_ref.at[:, span], sems.at[2 * i]),
            pltpu.make_async_copy(s_hbm.at[span, :], s_ref.at[span, :], sems.at[2 * i + 1]),
        ))
        for copy in copies[-1]:
            copy.start()
    image, halves = 0.0, []
    for i, both in enumerate(copies):
        for copy in both:
            copy.wait()
        halves.append(pair(z_ref[:, i * step : (i + 1) * step]))
        image = image + dot3(halves[i], pair(s_ref[i * step : (i + 1) * step, :]))
    turned = pair(image.T)
    for i, z in enumerate(halves):
        whole[:, i * step : (i + 1) * step] = dot3(turned, z)
    block = k // parts
    for i, r in enumerate(kept):
        keep_ref[i] = whole[:, pl.ds(place_of(axes, parts, block, r), block)]
        send_ref[i] = whole[:, pl.ds(place_of(axes, parts, block, r ^ 1), block)]


def first_kernel(s_ref, m_ref, out_ref, cols):
    n = s_ref.shape[1]
    s = s_ref[...]
    m_ref[:, :n] = dot(s.T, s)
    index = lax.broadcasted_iota(jnp.int32, (n, n), 0)
    other = lax.broadcasted_iota(jnp.int32, (n, n), 1)
    m_ref[:, n:] = jnp.where(index == other, 1.0, 0.0)
    eliminate(m_ref, out_ref, n, 0, n // 2, True, cols)


def second_kernel(m_ref, half_ref, z_ref, out_ref, total_ref, m, cols):
    n = m.shape[0]
    m[n // 2 :, :] = m_ref[n // 2 :, :]
    out_ref[: n // 2, :] = half_ref[: n // 2, :]
    eliminate(m, out_ref, n, n // 2, n, True, cols)
    z = z_ref[...]
    total_ref[...] = jnp.sum(z * z, axis=0, keepdims=True)


def shard_kernel(inverse_ref, *refs):
    total = refs[0][...]
    for ref in refs[1:-1]:
        total = total + ref[...]
    refs[-1][...] = dot(inverse_ref[...], total)


def products(axes, parts, numbers, z_ref, refs):
    block = refs[0].shape[2]
    y = jnp.concatenate([ref[i] for ref in refs for i in range(2)], axis=1)
    z = jnp.concatenate(
        [z_ref[:, pl.ds(place_of(axes, parts, block, r), block)] for r in numbers], axis=1
    )
    across = ((1,), (1,))
    return dot(y, y, across), dot3(pair(y), pair(z), across)


def near_kernel(axes, parts, kept, z_ref, near_ref, far_ref, m_ref):
    n = m_ref.shape[0]
    numbers = kept[:2] + [r ^ 1 for r in kept[:2]]
    m_ref[:, :n], m_ref[:, n:] = products(axes, parts, numbers, z_ref, (near_ref, far_ref))


def next_kernel(axes, parts, kept, z_ref, before_ref, near_ref, m_ref):
    n = m_ref.shape[0]
    gram, image = products(axes, parts, kept[2:], z_ref, (near_ref,))
    m_ref[:, :n] = before_ref[:, :n] + gram
    m_ref[:, n:] = before_ref[:, n:] + image


def last_kernel(axes, parts, kept, z_ref, near_ref, far_ref, total_ref, out_hbm, energy_ref, m, solved, out, cols, sems):
    n = near_ref.shape[0]
    gram, image = products(axes, parts, [r ^ 1 for r in kept[2:]], z_ref, (far_ref,))
    m[:, :n] = near_ref[:, :n] + gram
    m[:, n:] = near_ref[:, n:] + image
    half = n // 2
    copies, energy = [], 0.0
    for i in range(2):
        span = pl.ds(i * half, half)
        eliminate(m, solved, n, i * half, (i + 1) * half, False, cols)
        result = solved[i * half : (i + 1) * half, :]
        out[:, i * half : (i + 1) * half] = result.T
        copies.append(pltpu.make_async_copy(out.at[:, span], out_hbm.at[:, span], sems.at[i]))
        copies[i].start()
        energy = energy + jnp.sum(result * result)
    lane = lax.broadcasted_iota(jnp.int32, energy_ref.shape, 2)
    total = jnp.sum(total_ref[...])
    energy_ref[...] = jnp.where(lane == 0, energy, jnp.where(lane == 1, total, 0.0))
    for copy in copies:
        copy.wait()


def share_kernel(energy_ref, out_ref):
    sums = jnp.sum(energy_ref[:, 0, :], axis=0, keepdims=True)
    out_ref[...] = 1.0 - sums[:, 0:1] / sums[:, 1:2]


def call(kernel, outs, scratch, flops, limit, in_hbm=(), out_hbm=()):
    moved = 4 * sum(math.prod(s) for s in outs)

    def run(*args):
        return pl.pallas_call(
            kernel,
            out_shape=[jax.ShapeDtypeStruct(s, jnp.float32) for s in outs],
            in_specs=[HBM if i in in_hbm else VMEM for i in range(len(args))],
            out_specs=[HBM if i in out_hbm else VMEM for i in range(len(outs))],
            scratch_shapes=[
                pltpu.SemaphoreType.DMA((s,)) if isinstance(s, int) else pltpu.VMEM(s, jnp.float32)
                for s in scratch
            ],
            cost_estimate=pl.CostEstimate(flops=flops, bytes_accessed=moved, transcendentals=0),
            compiler_params=pltpu.CompilerParams(vmem_limit_bytes=limit * 2**20),
        )(*args)

    return run


def exchange(x, axis, size, mask):
    return lax.ppermute(x, axis, [(i, i ^ mask) for i in range(size)])


def steps_over(rows_size, grp_size, parts):
    masks = [(1 << i, 0) for i in range(parts.bit_length() - 1, rows_size.bit_length() - 1)]
    masks += [(1, 1 << i) for i in range(grp_size.bit_length() - 1)]

    def pairs(position):
        out = []
        for r in range(rows_size):
            for g in range(grp_size):
                odd = (r ^ bin(g).count("1")) & 1
                row_mask, grp_mask = masks[-1 - position] if odd else masks[position]
                out.append((r * grp_size + g, (r ^ row_mask) * grp_size + (g ^ grp_mask)))
        return out

    return [pairs(i) for i in range(len(masks))]


def local(rows_size, grp_size, factor, start_block):
    own, k = factor.shape
    n = start_block.shape[1]
    parts = 8
    assert rows_size % parts == 0 and k == parts * LANES
    block = k // parts
    half = parts // 2
    panel = (STRIP, PANEL, LANES)
    axes = ("rows", "grp")
    kept = [0] + [2 * i + 1 for i in range(1, half)]
    tie = lax.optimization_barrier
    apart = pltpu.with_memory_space_constraint

    keep, send = call(
        functools.partial(start_kernel, axes, parts, kept),
        [(half, n, block)] * 2, [(n, k), (own, k), (k, n), 2 * (k // min(k, 2 * LANES))], 10**8, 14, (0, 1),
    )(apart(factor, pltpu.HBM), apart(start_block, pltpu.HBM))
    got = exchange(send, "rows", rows_size, 1)
    pieces = [keep[i] + got[i] for i in range(half)]
    pieces[0], start_block = tie((pieces[0], start_block))
    moved = [exchange(pieces[i], "rows", rows_size, kept[i]) for i in range(1, half)]
    first = call(first_kernel, [(n, 2 * n), (n, n)], [panel], 10**10, 8)(start_block)
    first, moved = tie((first, moved))
    total = sum(moved, pieces[0])
    terms = [total]
    for i, pairs in enumerate(steps_over(rows_size, grp_size, parts)):
        total = sum(terms[1:], terms[0])
        other = lax.ppermute(total, axes, pairs)
        if i == 0:
            inverse, energy = call(second_kernel, [(n, n), (1, k)], [(n, 2 * n), panel], 5 * 10**9, 8)(*first, factor)
            inverse, other = tie((inverse, other))
        terms = [total, other]
    (shard,) = call(shard_kernel, [(n, block)], [], 10**8, 4)(inverse, *terms)

    arrived = []
    for r in kept[1:]:
        arrived.append(exchange(shard, "rows", rows_size, r))
    near = jnp.stack([shard, arrived[0]])
    far = exchange(near, "rows", rows_size, 1)
    (begun,) = call(functools.partial(near_kernel, axes, parts, kept), [(n, n + own)], [], 10**9, 8)(factor, near, far)
    begun, arrived[2] = tie((begun, arrived[2]))
    near = jnp.stack(arrived[1:])
    far = exchange(near, "rows", rows_size, 1)
    (begun,) = call(
        functools.partial(next_kernel, axes, parts, kept), [(n, n + own)], [], 10**9, 8
    )(factor, begun, near)
    begun, far = tie((begun, far))
    count = rows_size * grp_size
    compressed, energy = call(
        functools.partial(last_kernel, axes, parts, kept),
        [(own, n), (count, 1, LANES)], [(n, n + own), (n, own), (own, n), panel, 2], 10**10, 12, (), (0,),
    )(factor, begun, far, energy)
    energy = lax.all_to_all(energy, axes, 0, 0, tiled=True)
    (tail_share,) = call(share_kernel, [(1, 1)], [], 10**5, 4)(energy)
    return compressed, tail_share.reshape(())


def solution(mesh):
    def body(factor, start_block):
        return local(mesh.shape["rows"], mesh.shape["grp"], factor, start_block)

    return jax.shard_map(
        body,
        mesh=mesh,
        in_specs=(P(("rows", "grp"), None), P()),
        out_specs=(P(("rows", "grp"), None), P()),
        check_vma=False,
    )
```

```python
import functools
import math
import jax
import jax.numpy as jnp
from jax import lax
from jax.experimental import pallas as pl
from jax.experimental.pallas import tpu as pltpu
from jax.sharding import PartitionSpec as P

LANES = 128
PANEL = 32
STRIP = 16
EXACT = lax.Precision.HIGHEST
VMEM = pl.BlockSpec(memory_space=pltpu.VMEM)
HBM = pl.BlockSpec(memory_space=pltpu.HBM)


def dot(a, b, contract=((1,), (0,))):
    return lax.dot_general(
        a, b, (contract, ((), ())), precision=EXACT, preferred_element_type=jnp.float32
    )


def split3(x):
    high = x.astype(jnp.bfloat16)
    rest = x - high.astype(jnp.float32)
    mid = rest.astype(jnp.bfloat16)
    low = (rest - mid.astype(jnp.float32)).astype(jnp.bfloat16)
    return high, mid, low


def eliminate(m, out, n, first, last, lower, cols):
    width = m.shape[1]
    b = PANEL
    group = lax.broadcasted_iota(jnp.int32, (8, LANES), 0)
    for r0 in range(first, last, b):
        lo = r0 // LANES * LANES
        end = n + lo + LANES if lower else width
        chunks = list(range(lo, end, LANES))
        solved = [[] for _ in chunks]
        for c0 in range(r0, r0 + b, STRIP):
            tall = r0 + b - c0
            for j in range(STRIP):
                top = j // 8 * 8
                entry = m[c0 + top : r0 + b, c0 + j : c0 + j + 1]
                cols[j, top:tall, :] = jnp.broadcast_to(entry, (tall - top, LANES))
            units = [[] for _ in chunks]
            for base in range(0, STRIP, 8):
                column = [cols[base + j, base:tall, :] for j in range(8)]
                rows = [m[c0 + base : c0 + base + 8, q : q + LANES] for q in chunks]
                for i in range(base):
                    factor = cols[i, base:tall, :]
                    for j in range(8):
                        column[j] = column[j] - factor * cols[i, base + j : base + j + 1, :]
                    for q in range(len(chunks)):
                        rows[q] = rows[q] - factor[:8, :] * units[q][i]
                for j in range(8):
                    scale = lax.rsqrt(column[j][j : j + 1, :])
                    column[j] = column[j] * scale
                    for k in range(j + 1, 8):
                        column[k] = column[k] - column[j] * column[j][k : k + 1, :]
                    if base + 8 < tall:
                        cols[base + j, base:tall, :] = column[j]
                    below = jnp.where(group > j, column[j][:8, :], 0.0)
                    for q in range(len(chunks)):
                        unit = rows[q][j : j + 1, :] * scale
                        units[q].append(unit)
                        if j < 7:
                            rows[q] = rows[q] - below * unit
            for q, start in enumerate(chunks):
                solved[q].append(jnp.concatenate(units[q], axis=0))
                for top in range(STRIP, tall, 8):
                    lower_rows = m[c0 + top : c0 + top + 8, start : start + LANES]
                    for i in range(STRIP):
                        lower_rows = lower_rows - cols[i, top : top + 8, :] * units[q][i]
                    m[c0 + top : c0 + top + 8, start : start + LANES] = lower_rows
        panel = [jnp.concatenate(s, axis=0) for s in solved]
        for q, start in enumerate(chunks):
            if start >= n:
                out[r0 : r0 + b, start - n : start - n + LANES] = panel[q]
        if lower and end < width:
            out[r0 : r0 + b, end - n :] = jnp.zeros((b, width - end), jnp.float32)
        done = r0 + b
        if done < n:
            lo2 = done // LANES * LANES
            block = jnp.concatenate(panel[(lo2 - lo) // LANES :], axis=1)
            high, mid, low = split3(block)
            span = n - lo2
            left = jnp.concatenate([v[:, :span] for v in (high, high, mid, high, mid, low)], axis=0)
            right = jnp.concatenate([high, mid, high, low, mid, high], axis=0)
            update = lax.dot_general(
                left, right, (((0,), (0,)), ((), ())), preferred_element_type=jnp.float32
            )
            m[done:n, lo2:end] = m[done:n, lo2:end] - update[done - lo2 :, :]


def place_of(axes, parts, block, r):
    rows, grp = lax.axis_index(axes[0]), lax.axis_index(axes[1])
    flip = grp & 1
    for bit in range(1, 8):
        flip = flip ^ ((grp >> bit) & 1)
    me = (rows & (parts - 1)) ^ flip
    return pl.multiple_of((me ^ r) * block, LANES)


def pair(x):
    high = x.astype(jnp.bfloat16)
    return high, (x - high.astype(jnp.float32)).astype(jnp.bfloat16)


def dot3(a, b, contract=((1,), (0,))):
    (ah, al), (bh, bl) = a, b
    left = jnp.concatenate([ah, ah, al], axis=contract[0][0])
    right = jnp.concatenate([bh, bl, bh], axis=contract[1][0])
    return lax.dot_general(left, right, (contract, ((), ())), preferred_element_type=jnp.float32)


def start_kernel(axes, parts, kept, z_hbm, s_hbm, keep_ref, send_ref, whole, z_ref, s_ref, sems):
    k = z_ref.shape[1]
    step = min(k, 2 * LANES)
    copies = []
    for i in range(k // step):
        span = pl.ds(i * step, step)
        copies.append((
            pltpu.make_async_copy(z_hbm.at[:, span], z_ref.at[:, span], sems.at[2 * i]),
            pltpu.make_async_copy(s_hbm.at[span, :], s_ref.at[span, :], sems.at[2 * i + 1]),
        ))
        for copy in copies[-1]:
            copy.start()
    image, halves = 0.0, []
    for i, both in enumerate(copies):
        for copy in both:
            copy.wait()
        halves.append(pair(z_ref[:, i * step : (i + 1) * step]))
        image = image + dot3(halves[i], pair(s_ref[i * step : (i + 1) * step, :]))
    turned = pair(image.T)
    for i, z in enumerate(halves):
        whole[:, i * step : (i + 1) * step] = dot3(turned, z)
    block = k // parts
    for i, r in enumerate(kept):
        keep_ref[i] = whole[:, pl.ds(place_of(axes, parts, block, r), block)]
        send_ref[i] = whole[:, pl.ds(place_of(axes, parts, block, r ^ 1), block)]


def first_kernel(s_ref, m_ref, out_ref, cols):
    n = s_ref.shape[1]
    s = s_ref[...]
    m_ref[:, :n] = dot(s.T, s)
    index = lax.broadcasted_iota(jnp.int32, (n, n), 0)
    other = lax.broadcasted_iota(jnp.int32, (n, n), 1)
    m_ref[:, n:] = jnp.where(index == other, 1.0, 0.0)
    eliminate(m_ref, out_ref, n, 0, n // 2, True, cols)


def second_kernel(m_ref, half_ref, z_ref, out_ref, total_ref, m, cols):
    n = m.shape[0]
    m[n // 2 :, :] = m_ref[n // 2 :, :]
    out_ref[: n // 2, :] = half_ref[: n // 2, :]
    eliminate(m, out_ref, n, n // 2, n, True, cols)
    z = z_ref[...]
    total_ref[...] = jnp.sum(z * z, axis=0, keepdims=True)


def shard_kernel(inverse_ref, *refs):
    total = refs[0][...]
    for ref in refs[1:-1]:
        total = total + ref[...]
    refs[-1][...] = dot(inverse_ref[...], total)


def products(axes, parts, numbers, z_ref, refs):
    block = refs[0].shape[2]
    y = jnp.concatenate([ref[i] for ref in refs for i in range(2)], axis=1)
    z = jnp.concatenate(
        [z_ref[:, pl.ds(place_of(axes, parts, block, r), block)] for r in numbers], axis=1
    )
    across = ((1,), (1,))
    return dot(y, y, across), dot3(pair(y), pair(z), across)


def near_kernel(axes, parts, kept, z_ref, near_ref, far_ref, m_ref):
    n = m_ref.shape[0]
    numbers = kept[:2] + [r ^ 1 for r in kept[:2]]
    m_ref[:, :n], m_ref[:, n:] = products(axes, parts, numbers, z_ref, (near_ref, far_ref))


def next_kernel(axes, parts, kept, z_ref, before_ref, near_ref, m_ref):
    n = m_ref.shape[0]
    gram, image = products(axes, parts, kept[2:], z_ref, (near_ref,))
    m_ref[:, :n] = before_ref[:, :n] + gram
    m_ref[:, n:] = before_ref[:, n:] + image


def last_kernel(axes, parts, kept, z_ref, near_ref, far_ref, total_ref, out_hbm, energy_ref, rest_ref, m, solved, out, cols, sems):
    n = near_ref.shape[0]
    gram, image = products(axes, parts, [r ^ 1 for r in kept[2:]], z_ref, (far_ref,))
    m[:, :n] = near_ref[:, :n] + gram
    m[:, n:] = near_ref[:, n:] + image
    half = n // 2
    eliminate(m, solved, n, 0, half, False, cols)
    first = solved[:half, :]
    out[...] = first.T
    copy = pltpu.make_async_copy(out, out_hbm.at[:, pl.ds(0, half)], sems.at[0])
    copy.start()
    eliminate(m, solved, n, half, n, False, cols)
    second = solved[half:, :]
    rest_ref[...] = second
    energy = jnp.sum(first * first) + jnp.sum(second * second)
    lane = lax.broadcasted_iota(jnp.int32, energy_ref.shape, 2)
    total = jnp.sum(total_ref[...])
    energy_ref[...] = jnp.where(lane == 0, energy, jnp.where(lane == 1, total, 0.0))
    copy.wait()


def share_kernel(energy_ref, rest_ref, begun_hbm, out_hbm, share_ref, turned, sems):
    half = rest_ref.shape[0]
    turned[...] = rest_ref[...].T
    copy = pltpu.make_async_copy(turned, out_hbm.at[:, pl.ds(half, half)], sems.at[0])
    copy.start()
    sums = jnp.sum(energy_ref[:, 0, :], axis=0, keepdims=True)
    share_ref[...] = 1.0 - sums[:, 0:1] / sums[:, 1:2]
    copy.wait()


def call(kernel, outs, scratch, flops, limit, in_hbm=(), out_hbm=(), aliases=()):
    moved = 4 * sum(math.prod(s) for s in outs)

    def run(*args):
        return pl.pallas_call(
            kernel,
            out_shape=[jax.ShapeDtypeStruct(s, jnp.float32) for s in outs],
            in_specs=[HBM if i in in_hbm else VMEM for i in range(len(args))],
            out_specs=[HBM if i in out_hbm else VMEM for i in range(len(outs))],
            scratch_shapes=[
                pltpu.SemaphoreType.DMA((s,)) if isinstance(s, int) else pltpu.VMEM(s, jnp.float32)
                for s in scratch
            ],
            cost_estimate=pl.CostEstimate(flops=flops, bytes_accessed=moved, transcendentals=0),
            compiler_params=pltpu.CompilerParams(vmem_limit_bytes=limit * 2**20),
            input_output_aliases=dict(aliases),
        )(*args)

    return run


def exchange(x, axis, size, mask):
    return lax.ppermute(x, axis, [(i, i ^ mask) for i in range(size)])


def steps_over(rows_size, grp_size, parts):
    masks = [(1 << i, 0) for i in range(parts.bit_length() - 1, rows_size.bit_length() - 1)]
    masks += [(1, 1 << i) for i in range(grp_size.bit_length() - 1)]

    def pairs(position):
        out = []
        for r in range(rows_size):
            for g in range(grp_size):
                odd = (r ^ bin(g).count("1")) & 1
                row_mask, grp_mask = masks[-1 - position] if odd else masks[position]
                out.append((r * grp_size + g, (r ^ row_mask) * grp_size + (g ^ grp_mask)))
        return out

    return [pairs(i) for i in range(len(masks))]


def local(rows_size, grp_size, factor, start_block):
    own, k = factor.shape
    n = start_block.shape[1]
    parts = 8
    assert rows_size % parts == 0 and k == parts * LANES
    block = k // parts
    half = parts // 2
    panel = (STRIP, PANEL, LANES)
    axes = ("rows", "grp")
    kept = [0] + [2 * i + 1 for i in range(1, half)]
    tie = lax.optimization_barrier
    apart = pltpu.with_memory_space_constraint

    keep, send = call(
        functools.partial(start_kernel, axes, parts, kept),
        [(half, n, block)] * 2, [(n, k), (own, k), (k, n), 2 * (k // min(k, 2 * LANES))], 10**8, 14, (0, 1),
    )(apart(factor, pltpu.HBM), apart(start_block, pltpu.HBM))
    got = exchange(send, "rows", rows_size, 1)
    pieces = [keep[i] + got[i] for i in range(half)]
    pieces[0], start_block = tie((pieces[0], start_block))
    moved = [exchange(pieces[i], "rows", rows_size, kept[i]) for i in range(1, half)]
    first = call(first_kernel, [(n, 2 * n), (n, n)], [panel], 10**10, 8)(start_block)
    first, moved = tie((first, moved))
    total = sum(moved, pieces[0])
    terms = [total]
    for i, pairs in enumerate(steps_over(rows_size, grp_size, parts)):
        total = sum(terms[1:], terms[0])
        other = lax.ppermute(total, axes, pairs)
        if i == 0:
            inverse, energy = call(second_kernel, [(n, n), (1, k)], [(n, 2 * n), panel], 5 * 10**9, 8)(*first, factor)
            inverse, other = tie((inverse, other))
        terms = [total, other]
    (shard,) = call(shard_kernel, [(n, block)], [], 10**8, 4)(inverse, *terms)

    arrived = []
    for r in kept[1:]:
        arrived.append(exchange(shard, "rows", rows_size, r))
    near = jnp.stack([shard, arrived[0]])
    far = exchange(near, "rows", rows_size, 1)
    (begun,) = call(functools.partial(near_kernel, axes, parts, kept), [(n, n + own)], [], 10**9, 8)(factor, near, far)
    begun, arrived[2] = tie((begun, arrived[2]))
    near = jnp.stack(arrived[1:])
    far = exchange(near, "rows", rows_size, 1)
    (begun,) = call(
        functools.partial(next_kernel, axes, parts, kept), [(n, n + own)], [], 10**9, 8
    )(factor, begun, near)
    begun, far = tie((begun, far))
    count = rows_size * grp_size
    compressed, energy, rest = call(
        functools.partial(last_kernel, axes, parts, kept),
        [(own, n), (count, 1, LANES), (n // 2, own)], [(n, n + own), (n, own), (own, n // 2), panel, 1], 10**10, 12, (), (0,),
    )(factor, begun, far, energy)
    energy = lax.all_to_all(energy, axes, 0, 0, tiled=True)
    compressed, tail_share = call(
        share_kernel, [(own, n), (1, 1)], [(own, n // 2), 1], 10**5, 4, (2,), (0,), ((2, 0),)
    )(energy, rest, compressed)
    return compressed, tail_share.reshape(())


def solution(mesh):
    def body(factor, start_block):
        return local(mesh.shape["rows"], mesh.shape["grp"], factor, start_block)

    return jax.shard_map(
        body,
        mesh=mesh,
        in_specs=(P(("rows", "grp"), None), P()),
        out_specs=(P(("rows", "grp"), None), P()),
        check_vma=False,
    )
```
